32 devices in a mesh: patch: 16 (over z, y, x), batch: 2 (over core).
Axes of the slice: x: 2, y: 2, z: 4, core: 2. Of those that a mesh axis runs over, the one named last changes fastest.
Arguments:
- tokens: bfloat16 [4096, 1152], P(('batch', 'patch')), parts along dimension 0, may hold values from -6 to 6
- slots: int32 [4096], P(('batch', 'patch')), parts along dimension 0, may hold values from 0 to 127, as said below
- counts: int32 [32], P(('batch', 'patch')), parts along dimension 0, may hold values from 32 to 128, as said below
- shift: float32 [1152], replicated, may hold values from -3 to 3
- scale: float32 [1152], replicated, may hold values from -3 to 3
- gate: float32 [1152], replicated, may hold values from -4 to 4
- w_qkv: bfloat16 [1152, 3456], replicated, may hold values from -1 to 1
- w_out: bfloat16 [1152, 1152], replicated, may hold values from -0.1875 to 0.1875
Outputs:
- result: bfloat16 [4096, 1152], P(('batch', 'patch')), parts along dimension 0
The draws below stay inside these ranges and needn't reach their ends.
There are 2 independent parts, one for each index of `batch`. The reference program is written for one: setup_inputs(seed, part) draws one part's arguments, and reference() takes and returns one part's arrays. A program takes and returns all parts, laid end to end along the dimension named above; an argument that names none is the same for every part. Nothing has to cross between parts.
Inputs may be any that keep to these rules, and one draw needn't show every extreme that they name: `counts`: at least a quarter of each block's slots are live. The live slots of all blocks of an image number exactly 80 times the number of patch devices, and all blocks of some device are full. `slots`: every token's slot is below its block's count, and every slot below the count holds at least one token.
All inputs are finite; a program needn't handle non-finite values.
Results may differ from the reference program's by a relative error of at most 0.011.
Values may be sent and summed in bfloat16 or wider, within the bound.
A program may use at most 192 MiB of HBM per device.

```python
import jax
import jax.numpy as jnp
from jax import lax

D = 1152
HEADS = 16
HD = 72
BLK = 128
BLK_DEV = 1
TOKENS = 2048


def merge_plan(key):
    block_total = TOKENS // BLK
    device_total = block_total // BLK_DEV
    extra = BLK - BLK // 4
    needed = 5 * TOKENS // 8 - block_total * (BLK // 4)
    base = jax.random.fold_in(key, 11)
    key_level, key_full, key_noise, key_perm, key_rest = jax.random.split(base, 5)
    level = jax.random.randint(key_level, (block_total,), 0, 4096).astype(jnp.int32)
    chosen = jax.random.randint(key_full, (), 0, device_total).astype(jnp.int32)
    owner = jnp.arange(block_total, dtype=jnp.int32) // BLK_DEV
    level = jnp.where(owner == chosen, 8192, level).astype(jnp.int32)
    noise = jax.random.randint(key_noise, (block_total, extra), 0, 4096).astype(jnp.int32)
    ranked = ((level[:, None] + noise) * (block_total * extra)).reshape(block_total * extra) + jnp.arange(block_total * extra, dtype=jnp.int32)
    ordered = jnp.sort(ranked)
    cutoff = ordered[block_total * extra - needed]
    picked = (ranked >= cutoff).astype(jnp.int32).reshape(block_total, extra)
    counts = (BLK // 4 + jnp.sum(picked, axis=1)).astype(jnp.int32)
    ranks = jax.vmap(lambda k: jax.random.permutation(k, BLK))(jax.random.split(key_perm, block_total)).astype(jnp.int32)
    spare = jax.random.randint(key_rest, (block_total, BLK), 0, BLK * BLK).astype(jnp.int32) % counts[:, None]
    slots = jnp.where(ranks < counts[:, None], ranks, spare).astype(jnp.int32)
    return (slots.reshape(TOKENS), counts)


def draw_slots(key, part):
    return merge_plan(key)[0]


def draw_counts(key, part):
    return merge_plan(key)[1]


def draw_tokens(key, part):
    key_base = jax.random.fold_in(jax.random.fold_in(key, 23), 0)
    drawn = jnp.clip(jax.random.normal(key_base, (TOKENS, D), jnp.float32), -6.0, 6.0)
    return drawn.astype(jnp.bfloat16)


def draw_w_qkv(key, part):
    key_base = jax.random.fold_in(jax.random.fold_in(key, 37), 0)
    base = jnp.clip(jax.random.normal(key_base, (D, 3 * D), jnp.float32), -6.0, 6.0) * D ** (-0.5)
    return jnp.clip(base, -1.0, 1.0).astype(jnp.bfloat16)


def gaussian(own_key, extent, deviation, limit, kind=jnp.bfloat16):
    drawn = jax.random.normal(own_key, extent, jnp.float32) * deviation
    return jnp.minimum(jnp.maximum(drawn, -limit), limit).astype(kind)


def setup_inputs(seed: int = 0, part: int = 0) -> dict:
    key_of = jax.random.split(jax.random.key(seed), 9)
    part_splits = jax.random.split(jax.random.fold_in(key_of[8], part), 9)
    tokens = draw_tokens(jax.random.fold_in(jax.random.fold_in(key_of[8], part), 71), part)
    slots = draw_slots(jax.random.fold_in(jax.random.fold_in(key_of[8], part), 71), part)
    counts = draw_counts(jax.random.fold_in(jax.random.fold_in(key_of[8], part), 71), part)
    shift = gaussian(key_of[3], (D,), 0.5, 3.0, jnp.float32)
    scale = gaussian(key_of[4], (D,), 0.5, 3.0, jnp.float32)
    gate = gaussian(key_of[5], (D,), 1.0, 4.0, jnp.float32)
    w_qkv = draw_w_qkv(jax.random.fold_in(key_of[8], 71), part)
    w_out = gaussian(key_of[7], (D, D), D ** -0.5, 0.1875)
    return dict(tokens=tokens, slots=slots, counts=counts, shift=shift, scale=scale, gate=gate, w_qkv=w_qkv, w_out=w_out)


def layer_norm(merged, shift, scale):
    values = merged.astype(jnp.float32)
    center = lax.optimization_barrier(jnp.mean(values, axis=-1, keepdims=True))
    spread = lax.optimization_barrier(jnp.mean((values - center) ** 2, axis=-1, keepdims=True))
    return ((values - center) * lax.rsqrt(spread + 1e-06) * (1.0 + scale) + shift).astype(jnp.bfloat16)

def reference(tokens, slots, counts, shift, scale, gate, w_qkv, w_out):
    nblk = TOKENS // BLK
    onehot = (slots.reshape(nblk, BLK)[:, :, None] == jnp.arange(BLK, dtype=jnp.int32)[None, None, :]).astype(jnp.float32)
    sums = jnp.einsum('bts,btd->bsd', onehot, tokens.reshape(nblk, BLK, D).astype(jnp.float32))
    members = lax.optimization_barrier(jnp.sum(onehot, axis=1))
    merged = (sums / jnp.maximum(members, 1.0)[:, :, None]).astype(jnp.bfloat16).reshape(TOKENS, D)
    normed = layer_norm(merged, shift, scale)
    qkv = jnp.dot(normed, w_qkv, preferred_element_type=jnp.float32)
    query = qkv[:, :D].astype(jnp.bfloat16).reshape(TOKENS, HEADS, HD).transpose(1, 0, 2)
    keys = qkv[:, D:2 * D].astype(jnp.bfloat16).reshape(TOKENS, HEADS, HD).transpose(1, 0, 2)
    values = qkv[:, 2 * D:].astype(jnp.bfloat16).reshape(TOKENS, HEADS, HD).transpose(1, 0, 2)
    live = (jnp.arange(BLK, dtype=jnp.int32)[None, :] < counts[:, None]).reshape(TOKENS)
    bias = jnp.where(live, jnp.log(jnp.maximum(members.reshape(TOKENS), 1.0)), -1e+30).astype(jnp.float32)
    inverse = 1.0 / HD ** 0.5

    def one_head(items):
        qh, kh, vh = items
        score = jnp.dot(qh, kh.T, preferred_element_type=jnp.float32) * inverse + bias[None, :]
        top = lax.optimization_barrier(jnp.max(score, axis=-1, keepdims=True))
        probs = jnp.exp(score - top)
        total = lax.optimization_barrier(jnp.sum(probs, axis=-1, keepdims=True))
        return jnp.dot(probs.astype(jnp.bfloat16), vh, preferred_element_type=jnp.float32) / total
    heads_out = lax.map(one_head, (query, keys, values))
    attended = heads_out.transpose(1, 0, 2).reshape(TOKENS, D).astype(jnp.bfloat16)
    projected = jnp.dot(attended, w_out, preferred_element_type=jnp.float32)
    branch = jnp.einsum('bts,bsd->btd', onehot, projected.reshape(nblk, BLK, D), precision=lax.Precision.HIGHEST).reshape(TOKENS, D)
    return (tokens.astype(jnp.float32) + gate * branch).astype(jnp.bfloat16)
```

```python
import functools
import math

import jax
import jax.numpy as jnp
from jax import lax
from jax.experimental import pallas as pl
from jax.experimental.pallas import tpu as pltpu
from jax.sharding import PartitionSpec as P

HEADS = 16
BLK = 128
AUG = 8
CHUNK = 384
MESH = pl.DeviceIdType.MESH


def layer_norm(merged, shift, scale):
    values = merged.astype(jnp.float32)
    center = jnp.mean(values, axis=-1, keepdims=True)
    spread = jnp.mean((values - center) ** 2, axis=-1, keepdims=True)
    return ((values - center) * lax.rsqrt(spread + 1e-06) * (1.0 + scale) + shift).astype(
        jnp.bfloat16
    )


def merge(tokens, slots, counts):
    rows, width = tokens.shape
    nblk = rows // BLK
    onehot = slots.reshape(nblk, BLK)[:, :, None] == jnp.arange(BLK, dtype=jnp.int32)[None, None, :]
    sums = jnp.einsum(
        "bts,btd->bsd",
        onehot.astype(jnp.bfloat16),
        tokens.reshape(nblk, BLK, width),
        preferred_element_type=jnp.float32,
    )
    members = jnp.sum(onehot.astype(jnp.float32), axis=1)
    merged = (
        (sums / jnp.maximum(members, 1.0)[:, :, None]).astype(jnp.bfloat16).reshape(rows, width)
    )
    alive = (jnp.arange(BLK, dtype=jnp.int32)[None, :] < counts[:, None]).reshape(rows)
    bias = jnp.where(alive, jnp.log(jnp.maximum(members, 1.0)).reshape(rows), -1e30)
    return onehot, merged, bias


def attention(
    n, hd, slots, counts, tokens, shift, scale, w_hbm, out, w, turned, kq_msg, v_msg,
    kq_in, v_in, qs, ks, vs, probs, part, w_sem, *sems
):
    kq_out_sem, kq_in_sem, v_out_sem, v_in_sem, r_out_sem, r_in_sem = sems
    me = lax.axis_index("patch")
    rows, width = tokens.shape
    aug = hd + AUG

    def weights(p):
        return pltpu.make_async_copy(w_hbm.at[:, pl.ds(p * width, width)], w.at[p], w_sem.at[p])

    for p in (1, 0, 2):
        weights(p).start()
    barrier = pltpu.get_barrier_semaphore()
    for i in range(1, n):
        pl.semaphore_signal(
            barrier, inc=1, device_id={"patch": lax.rem(me + i, n)}, device_id_type=MESH
        )

    onehot = slots[...] == lax.broadcasted_iota(jnp.int32, (rows, rows), 0)
    exact = onehot.astype(jnp.float32)
    picks = exact.astype(jnp.bfloat16)
    sums = jnp.dot(picks, tokens[...], preferred_element_type=jnp.float32)
    members = jnp.sum(exact, axis=1, keepdims=True)
    merged = (sums / jnp.maximum(members, 1.0)).astype(jnp.bfloat16)
    normed = layer_norm(merged, shift[...], scale[...])
    sizes = lax.dot_general(
        jnp.ones((AUG, rows), jnp.bfloat16),
        picks,
        (((1,), (1,)), ((), ())),
        preferred_element_type=jnp.float32,
    )
    alive = lax.broadcasted_iota(jnp.int32, (AUG, rows), 1) < counts[...]
    lift = jnp.where(alive, jnp.log(jnp.maximum(sizes, 1.0)), -1e30) * math.sqrt(hd)
    high = lift.astype(jnp.bfloat16).astype(jnp.float32)
    rest = lift - high
    middle = rest.astype(jnp.bfloat16).astype(jnp.float32)
    low = rest - middle
    line = lax.broadcasted_iota(jnp.int32, (AUG, rows), 0)
    extra = jnp.where(
        line == 0, high, jnp.where(line == 1, middle, jnp.where(line == 2, low, 0.0))
    )

    def project(p):
        weights(p).wait()
        for at in range(0, width, CHUNK):
            piece = jnp.dot(normed, w[p, :, at : at + CHUNK], preferred_element_type=jnp.float32)
            turned[at : at + CHUNK] = piece.T

    def head(h):
        return turned[h * hd : (h + 1) * hd]

    project(1)
    for h in range(n):
        kq_msg[h, :aug] = jnp.concatenate([head(h), extra], axis=0).astype(jnp.bfloat16)
    project(0)
    for h in range(n):
        kq_msg[h, aug:] = head(h).astype(jnp.bfloat16)

    def copy(src_ref, dst_ref, send, recv, dst, src):
        return pltpu.make_async_remote_copy(
            src_ref=src_ref.at[dst],
            dst_ref=dst_ref.at[src],
            send_sem=send.at[dst],
            recv_sem=recv.at[src],
            device_id={"patch": dst},
            device_id_type=MESH,
        )

    def kq_to(dst, src):
        return copy(kq_msg, kq_in, kq_out_sem, kq_in_sem, dst, src)

    def v_to(dst, src):
        return copy(v_msg, v_in, v_out_sem, v_in_sem, dst, src)

    def result_to(dst, src):
        return copy(part, out, r_out_sem, r_in_sem, dst, src)

    pl.semaphore_wait(barrier, n - 1)
    for i in range(1, n):
        kq_to(lax.rem(me + i, n), me).start()
    project(2)
    for h in range(n):
        v_msg[h] = head(h).astype(jnp.bfloat16)
    for i in range(1, n):
        v_to(lax.rem(me + i, n), me).start()

    tail = jnp.ones((AUG, rows), jnp.bfloat16)

    def columns(src):
        return pl.ds(pl.multiple_of(src * rows, rows), rows)

    def place_kq(src, block):
        ks[:, columns(src)] = block[:aug]
        qs[:, columns(src)] = jnp.concatenate([block[aug:], tail], axis=0)

    def place_v(src, block):
        vs[:, columns(src)] = jnp.concatenate([block, tail], axis=0)

    place_kq(me, kq_msg[me])
    for i in range(1, n):
        src = lax.rem(me + n - i, n)
        kq_to(src, src).wait_recv()
        place_kq(src, kq_in[src])

    factor = math.log2(math.e) / math.sqrt(hd)
    wide = 2 * rows
    pairs = n // 2

    def pair_of(c):
        return lax.rem(me // 2 + c, pairs)

    def send_pair(c):
        for t in range(2):
            dst = 2 * pair_of(c) + t

            @pl.when(dst != me)
            def _():
                result_to(dst, me).start()

            @pl.when(dst == me)
            def _():
                out[me] = part[me]

    def weigh(c, _):
        query = qs[:, pl.ds(pl.multiple_of(pair_of(c) * wide, wide), wide)]
        score = lax.dot_general(
            ks[...], query, (((0,), (0,)), ((), ())), preferred_element_type=jnp.float32
        )
        top = jnp.max(score, axis=0, keepdims=True)
        probs[c] = jnp.exp2((score - top) * factor).astype(jnp.bfloat16)
        return 0

    lax.fori_loop(0, pairs, weigh, 0)

    place_v(me, v_msg[me])
    for i in range(1, n):
        src = lax.rem(me + n - i, n)
        v_to(src, src).wait_recv()
        place_v(src, v_in[src])

    def finish(c, _):
        first = pair_of(c)
        acc = jnp.dot(vs[...], probs[c], preferred_element_type=jnp.float32)
        done = (acc[:hd] / acc[hd : hd + 1]).astype(jnp.bfloat16)
        part[2 * first] = done[:, :rows]
        part[2 * first + 1] = done[:, rows:]

        @pl.when(c > 0)
        def _():
            send_pair(c - 1)

        return 0

    lax.fori_loop(0, pairs, finish, 0)
    send_pair(pairs - 1)

    for i in range(1, n):
        other = lax.rem(me + i, n)
        kq_to(other, me).wait_send()
        v_to(other, me).wait_send()
        result_to(other, me).wait_send()
        src = lax.rem(me + n - i, n)
        result_to(src, src).wait_recv()


def heads_apart(n, width, tokens, slots, counts, shift, scale, gate, w_qkv, w_out):
    rows = tokens.shape[0]
    hd = width // HEADS
    aug = hd + AUG
    vmem = pl.BlockSpec(memory_space=pltpu.VMEM)
    attended = pl.pallas_call(
        functools.partial(attention, n, hd),
        out_shape=jax.ShapeDtypeStruct((n, hd, rows), jnp.bfloat16),
        in_specs=[vmem] * 5 + [pl.BlockSpec(memory_space=pl.ANY)],
        out_specs=vmem,
        scratch_shapes=[
            pltpu.VMEM((3, width, width), jnp.bfloat16),
            pltpu.VMEM((width, rows), jnp.float32),
            pltpu.VMEM((n, aug + hd, rows), jnp.bfloat16),
            pltpu.VMEM((n, hd, rows), jnp.bfloat16),
            pltpu.VMEM((n, aug + hd, rows), jnp.bfloat16),
            pltpu.VMEM((n, hd, rows), jnp.bfloat16),
            pltpu.VMEM((aug, n * rows), jnp.bfloat16),
            pltpu.VMEM((aug, n * rows), jnp.bfloat16),
            pltpu.VMEM((aug, n * rows), jnp.bfloat16),
            pltpu.VMEM((n // 2, n * rows, 2 * rows), jnp.bfloat16),
            pltpu.VMEM((n, hd, rows), jnp.bfloat16),
            pltpu.SemaphoreType.DMA((3,)),
        ]
        + [pltpu.SemaphoreType.DMA((n,))] * 6,
        compiler_params=pltpu.CompilerParams(
            collective_id=0, has_side_effects=True, vmem_limit_bytes=56 * 1024 * 1024
        ),
    )(slots[None], counts[None], tokens, shift[None], scale[None], w_qkv)
    attended = attended.reshape(width, rows)
    onehot = slots[:, None] == jnp.arange(rows, dtype=jnp.int32)[None, :]
    picked = lax.dot_general(
        onehot.astype(jnp.bfloat16),
        attended,
        (((1,), (1,)), ((), ())),
        preferred_element_type=jnp.float32,
    ).astype(jnp.bfloat16)
    branch = jnp.dot(picked, w_out, preferred_element_type=jnp.float32)
    return (tokens.astype(jnp.float32) + gate * branch).astype(jnp.bfloat16)


def rows_gathered(tokens, slots, counts, shift, scale, gate, w_qkv, w_out):
    rows, width = tokens.shape
    nblk = rows // BLK
    hd = width // HEADS
    onehot, merged, bias = merge(tokens, slots, counts)
    normed = layer_norm(merged, shift, scale)
    qkv = jnp.dot(normed, w_qkv, preferred_element_type=jnp.float32)
    query, keys, values = (
        qkv[:, i * width : (i + 1) * width].astype(jnp.bfloat16) for i in range(3)
    )
    keys = lax.all_gather(keys, "patch", axis=0, tiled=True).reshape(-1, HEADS, hd)
    values = lax.all_gather(values, "patch", axis=0, tiled=True).reshape(-1, HEADS, hd)
    bias = lax.all_gather(bias, "patch", axis=0, tiled=True)
    query = query.reshape(rows, HEADS, hd)
    score = jnp.einsum("qhe,khe->hqk", query, keys, preferred_element_type=jnp.float32)
    score = score / hd**0.5 + bias[None, None, :]
    probs = jnp.exp(score - jnp.max(score, axis=-1, keepdims=True))
    total = jnp.sum(probs, axis=-1)
    update = jnp.einsum(
        "hqk,khe->hqe", probs.astype(jnp.bfloat16), values, preferred_element_type=jnp.float32
    )
    attended = (update / total[:, :, None]).transpose(1, 0, 2).reshape(rows, width)
    picked = jnp.einsum(
        "bts,bsd->btd",
        onehot.astype(jnp.bfloat16),
        attended.astype(jnp.bfloat16).reshape(nblk, BLK, width),
        preferred_element_type=jnp.float32,
    ).astype(jnp.bfloat16)
    branch = jnp.dot(picked.reshape(rows, width), w_out, preferred_element_type=jnp.float32)
    return (tokens.astype(jnp.float32) + gate * branch).astype(jnp.bfloat16)


def solution(mesh):
    n = mesh.shape["patch"]

    def body(tokens, *rest):
        if n == HEADS and tokens.shape[0] == BLK:
            return heads_apart(n, tokens.shape[1], tokens, *rest)
        return rows_gathered(tokens, *rest)

    return jax.shard_map(
        body,
        mesh=mesh,
        in_specs=(
            P(("batch", "patch"), None),
            P(("batch", "patch")),
            P(("batch", "patch")),
            P(),
            P(),
            P(),
            P(),
            P(),
        ),
        out_specs=P(("batch", "patch"), None),
        check_vma=False,
    )
```

```python
import functools
import math

import jax
import jax.numpy as jnp
from jax import lax
from jax.experimental import pallas as pl
from jax.experimental.pallas import tpu as pltpu
from jax.sharding import PartitionSpec as P

HEADS = 16
BLK = 128
AUG = 8
CHUNK = 384
MESH = pl.DeviceIdType.MESH


def layer_norm(merged, shift, scale):
    values = merged.astype(jnp.float32)
    center = jnp.mean(values, axis=-1, keepdims=True)
    spread = jnp.mean((values - center) ** 2, axis=-1, keepdims=True)
    return ((values - center) * lax.rsqrt(spread + 1e-06) * (1.0 + scale) + shift).astype(
        jnp.bfloat16
    )


def merge(tokens, slots, counts):
    rows, width = tokens.shape
    nblk = rows // BLK
    onehot = slots.reshape(nblk, BLK)[:, :, None] == jnp.arange(BLK, dtype=jnp.int32)[None, None, :]
    sums = jnp.einsum(
        "bts,btd->bsd",
        onehot.astype(jnp.bfloat16),
        tokens.reshape(nblk, BLK, width),
        preferred_element_type=jnp.float32,
    )
    members = jnp.sum(onehot.astype(jnp.float32), axis=1)
    merged = (
        (sums / jnp.maximum(members, 1.0)[:, :, None]).astype(jnp.bfloat16).reshape(rows, width)
    )
    alive = (jnp.arange(BLK, dtype=jnp.int32)[None, :] < counts[:, None]).reshape(rows)
    bias = jnp.where(alive, jnp.log(jnp.maximum(members, 1.0)).reshape(rows), -1e30)
    return onehot, merged, bias


def attention(
    n, hd, slots, counts, tokens, shift, scale, w_hbm, out, w, turned, kq_msg, v_msg,
    kq_in, v_in, qs, ks, vs, probs, part, w_sem, *sems
):
    kq_out_sem, kq_in_sem, v_out_sem, v_in_sem, r_out_sem, r_in_sem = sems
    me = lax.axis_index("patch")
    rows, width = tokens.shape
    aug = hd + AUG

    def weights(p):
        return pltpu.make_async_copy(w_hbm.at[:, pl.ds(p * width, width)], w.at[p], w_sem.at[p])

    for p in (1, 0, 2):
        weights(p).start()
    barrier = pltpu.get_barrier_semaphore()
    for i in range(1, n):
        pl.semaphore_signal(
            barrier, inc=1, device_id={"patch": lax.rem(me + i, n)}, device_id_type=MESH
        )

    onehot = slots[...] == lax.broadcasted_iota(jnp.int32, (rows, rows), 0)
    exact = onehot.astype(jnp.float32)
    picks = exact.astype(jnp.bfloat16)
    sums = jnp.dot(picks, tokens[...], preferred_element_type=jnp.float32)
    members = jnp.sum(exact, axis=1, keepdims=True)
    merged = (sums / jnp.maximum(members, 1.0)).astype(jnp.bfloat16)
    normed = layer_norm(merged, shift[...][None], scale[...][None])
    sizes = lax.dot_general(
        jnp.ones((AUG, rows), jnp.bfloat16),
        picks,
        (((1,), (1,)), ((), ())),
        preferred_element_type=jnp.float32,
    )
    alive = lax.broadcasted_iota(jnp.int32, (AUG, rows), 1) < counts[...]
    lift = jnp.where(alive, jnp.log(jnp.maximum(sizes, 1.0)), -1e30) * math.sqrt(hd)
    high = lift.astype(jnp.bfloat16).astype(jnp.float32)
    rest = lift - high
    middle = rest.astype(jnp.bfloat16).astype(jnp.float32)
    low = rest - middle
    line = lax.broadcasted_iota(jnp.int32, (AUG, rows), 0)
    extra = jnp.where(
        line == 0, high, jnp.where(line == 1, middle, jnp.where(line == 2, low, 0.0))
    )

    def project(p):
        weights(p).wait()
        for at in range(0, width, CHUNK):
            piece = jnp.dot(normed, w[p, :, at : at + CHUNK], preferred_element_type=jnp.float32)
            turned[at : at + CHUNK] = piece.T

    def head(h):
        return turned[h * hd : (h + 1) * hd]

    project(1)
    for h in range(n):
        kq_msg[h, :aug] = jnp.concatenate([head(h), extra], axis=0).astype(jnp.bfloat16)
    project(0)
    for h in range(n):
        kq_msg[h, aug:] = head(h).astype(jnp.bfloat16)

    def copy(src_ref, dst_ref, send, recv, dst, src):
        return pltpu.make_async_remote_copy(
            src_ref=src_ref.at[dst],
            dst_ref=dst_ref.at[src],
            send_sem=send.at[dst],
            recv_sem=recv.at[src],
            device_id={"patch": dst},
            device_id_type=MESH,
        )

    def kq_to(dst, src):
        return copy(kq_msg, kq_in, kq_out_sem, kq_in_sem, dst, src)

    def v_to(dst, src):
        return copy(v_msg, v_in, v_out_sem, v_in_sem, dst, src)

    def result_to(dst, src):
        return copy(part, out, r_out_sem, r_in_sem, dst, src)

    pl.semaphore_wait(barrier, n - 1)
    for i in range(1, n):
        kq_to(lax.rem(me + i, n), me).start()
    project(2)
    for h in range(n):
        v_msg[h] = head(h).astype(jnp.bfloat16)
    for i in range(1, n):
        v_to(lax.rem(me + i, n), me).start()

    tail = jnp.ones((AUG, rows), jnp.bfloat16)

    def columns(src):
        return pl.ds(pl.multiple_of(src * rows, rows), rows)

    def place_kq(src, block):
        ks[:, columns(src)] = block[:aug]
        qs[:, columns(src)] = jnp.concatenate([block[aug:], tail], axis=0)

    def place_v(src, block):
        vs[:, columns(src)] = jnp.concatenate([block, tail], axis=0)

    place_kq(me, kq_msg[me])
    for i in range(1, n):
        src = lax.rem(me + n - i, n)
        kq_to(src, src).wait_recv()
        place_kq(src, kq_in[src])

    factor = math.log2(math.e) / math.sqrt(hd)
    wide = 2 * rows
    pairs = n // 2

    def pair_of(c):
        return lax.rem(me // 2 + c, pairs)

    def send_pair(c):
        for t in range(2):
            dst = 2 * pair_of(c) + t

            @pl.when(dst != me)
            def _():
                result_to(dst, me).start()

            @pl.when(dst == me)
            def _():
                out[me] = part[me]

    def weigh(c, _):
        query = qs[:, pl.ds(pl.multiple_of(pair_of(c) * wide, wide), wide)]
        score = lax.dot_general(
            ks[...], query, (((0,), (0,)), ((), ())), preferred_element_type=jnp.float32
        )
        top = jnp.max(score, axis=0, keepdims=True)
        probs[c] = jnp.exp2((score - top) * factor).astype(jnp.bfloat16)
        return 0

    lax.fori_loop(0, pairs, weigh, 0)

    place_v(me, v_msg[me])
    for i in range(1, n):
        src = lax.rem(me + n - i, n)
        v_to(src, src).wait_recv()
        place_v(src, v_in[src])

    def finish(c, _):
        first = pair_of(c)
        acc = jnp.dot(vs[...], probs[c], preferred_element_type=jnp.float32)
        done = (acc[:hd] / acc[hd : hd + 1]).astype(jnp.bfloat16)
        part[2 * first] = done[:, :rows]
        part[2 * first + 1] = done[:, rows:]

        @pl.when(c > 0)
        def _():
            send_pair(c - 1)

        return 0

    lax.fori_loop(0, pairs, finish, 0)
    send_pair(pairs - 1)

    for i in range(1, n):
        other = lax.rem(me + i, n)
        kq_to(other, me).wait_send()
        v_to(other, me).wait_send()
        result_to(other, me).wait_send()
        src = lax.rem(me + n - i, n)
        result_to(src, src).wait_recv()


def heads_apart(n, width, tokens, slots, counts, shift, scale, gate, w_qkv, w_out):
    rows = tokens.shape[0]
    hd = width // HEADS
    aug = hd + AUG
    vmem = pl.BlockSpec(memory_space=pltpu.VMEM)
    attended = pl.pallas_call(
        functools.partial(attention, n, hd),
        out_shape=jax.ShapeDtypeStruct((n, hd, rows), jnp.bfloat16),
        in_specs=[vmem] * 5 + [pl.BlockSpec(memory_space=pl.ANY)],
        out_specs=vmem,
        scratch_shapes=[
            pltpu.VMEM((3, width, width), jnp.bfloat16),
            pltpu.VMEM((width, rows), jnp.float32),
            pltpu.VMEM((n, aug + hd, rows), jnp.bfloat16),
            pltpu.VMEM((n, hd, rows), jnp.bfloat16),
            pltpu.VMEM((n, aug + hd, rows), jnp.bfloat16),
            pltpu.VMEM((n, hd, rows), jnp.bfloat16),
            pltpu.VMEM((aug, n * rows), jnp.bfloat16),
            pltpu.VMEM((aug, n * rows), jnp.bfloat16),
            pltpu.VMEM((aug, n * rows), jnp.bfloat16),
            pltpu.VMEM((n // 2, n * rows, 2 * rows), jnp.bfloat16),
            pltpu.VMEM((n, hd, rows), jnp.bfloat16),
            pltpu.SemaphoreType.DMA((3,)),
        ]
        + [pltpu.SemaphoreType.DMA((n,))] * 6,
        compiler_params=pltpu.CompilerParams(
            collective_id=0, has_side_effects=True, vmem_limit_bytes=56 * 1024 * 1024
        ),
    )(slots[None], counts[None], tokens, shift, scale, w_qkv)
    attended = attended.reshape(width, rows)
    onehot = slots[:, None] == jnp.arange(rows, dtype=jnp.int32)[None, :]
    picked = lax.dot_general(
        onehot.astype(jnp.bfloat16),
        attended,
        (((1,), (1,)), ((), ())),
        preferred_element_type=jnp.float32,
    ).astype(jnp.bfloat16)
    branch = jnp.dot(picked, w_out, preferred_element_type=jnp.float32)
    return (tokens.astype(jnp.float32) + gate * branch).astype(jnp.bfloat16)


def rows_gathered(tokens, slots, counts, shift, scale, gate, w_qkv, w_out):
    rows, width = tokens.shape
    nblk = rows // BLK
    hd = width // HEADS
    onehot, merged, bias = merge(tokens, slots, counts)
    normed = layer_norm(merged, shift, scale)
    qkv = jnp.dot(normed, w_qkv, preferred_element_type=jnp.float32)
    query, keys, values = (
        qkv[:, i * width : (i + 1) * width].astype(jnp.bfloat16) for i in range(3)
    )
    keys = lax.all_gather(keys, "patch", axis=0, tiled=True).reshape(-1, HEADS, hd)
    values = lax.all_gather(values, "patch", axis=0, tiled=True).reshape(-1, HEADS, hd)
    bias = lax.all_gather(bias, "patch", axis=0, tiled=True)
    query = query.reshape(rows, HEADS, hd)
    score = jnp.einsum("qhe,khe->hqk", query, keys, preferred_element_type=jnp.float32)
    score = score / hd**0.5 + bias[None, None, :]
    probs = jnp.exp(score - jnp.max(score, axis=-1, keepdims=True))
    total = jnp.sum(probs, axis=-1)
    update = jnp.einsum(
        "hqk,khe->hqe", probs.astype(jnp.bfloat16), values, preferred_element_type=jnp.float32
    )
    attended = (update / total[:, :, None]).transpose(1, 0, 2).reshape(rows, width)
    picked = jnp.einsum(
        "bts,bsd->btd",
        onehot.astype(jnp.bfloat16),
        attended.astype(jnp.bfloat16).reshape(nblk, BLK, width),
        preferred_element_type=jnp.float32,
    ).astype(jnp.bfloat16)
    branch = jnp.dot(picked.reshape(rows, width), w_out, preferred_element_type=jnp.float32)
    return (tokens.astype(jnp.float32) + gate * branch).astype(jnp.bfloat16)


def solution(mesh):
    n = mesh.shape["patch"]

    def body(tokens, *rest):
        if n == HEADS and tokens.shape[0] == BLK:
            return heads_apart(n, tokens.shape[1], tokens, *rest)
        return rows_gathered(tokens, *rest)

    return jax.shard_map(
        body,
        mesh=mesh,
        in_specs=(
            P(("batch", "patch"), None),
            P(("batch", "patch")),
            P(("batch", "patch")),
            P(),
            P(),
            P(),
            P(),
            P(),
        ),
        out_specs=P(("batch", "patch"), None),
        check_vma=False,
    )
```
